1024 devices in a mesh: dp: 64 (over x, z), tensor: 8 (over y), pipe: 2 (over core).
Axes of the slice: x: 4, y: 8, z: 16, core: 2. Of those that a mesh axis runs over, the one named last changes fastest.
Arguments:
- patches: bfloat16 [1280, 49152], P('tensor', ('dp', 'pipe')), may hold values from -6 to 6
- lengths: int32 [6144], P(('dp', 'pipe')), may hold values from 1 to 8
- slot_plan: int32 [6144], P(('dp', 'pipe')), may hold values from 0 to 63, as said below
- starts: int32 [8192], P(('dp', 'pipe')), may hold values from 0 to 756, as said below
- text_rows: bfloat16 [1280, 98304], P('tensor', ('dp', 'pipe')), may hold values from -6 to 6
- cotangent: bfloat16 [1280, 98304], P('tensor', ('dp', 'pipe')), may hold values from -24 to 24
- ln_gain: float32 [1280], replicated, may hold values from 0.25 to 1.75
- ln_bias: float32 [1280], replicated, may hold values from -3 to 3
- w_qkv: bfloat16 [3, 1280, 1280], P(None, 'tensor'), may hold values from -0.15625 to 0.15625
- w_out: bfloat16 [1280, 1280], P('tensor'), may hold values from -0.15625 to 0.15625
Outputs:
- features: bfloat16 [1280, 98304], P('tensor', ('dp', 'pipe'))
- weight_grad: float32 [1280, 1280], P('tensor', ('dp', 'pipe'))
The draws below stay inside these ranges and needn't reach their ends.
Inputs may be any that keep to these rules, and one draw needn't show every extreme that they name: `slot_plan`: the 48 images of one data group have distinct slots. `starts`: within each data group the 64 places' blocks of 8 positions rise and are disjoint, separated by 0 to 4 positions, and lie inside the group's 768 positions.
All inputs are finite; a program needn't handle non-finite values.
Results may differ from the reference program's by a relative error of at most 0.0073.
Values may be sent and summed in bfloat16 or wider, within the bound.
A program may use at most 32 MiB of HBM per device.

```python
import math
import jax
import jax.numpy as jnp
from jax import lax

D = 1280
HEADS = 16
HEAD_DIM = 80
LEN = 8
IMG_DEV = 48
GAP = 4
CAP = 1
SLOTS = 64
SEQ_DEV = 768
IMAGES = 6144
SEQ = 98304
N_DP = 64
N_TENSOR = 8
N_PIPE = 2


def draw_slot_plan(key, part):
    group_keys = jax.random.split(jax.random.fold_in(key, 11), N_DP * N_PIPE)

    def one_group(group_key):
        return jax.random.permutation(group_key, SLOTS)[:IMG_DEV]
    return jax.vmap(one_group)(group_keys).reshape(-1).astype(jnp.int32)


def draw_starts(key, part):
    spacing = jax.random.randint(jax.random.fold_in(key, 23), (N_DP * N_PIPE, SLOTS), 0, GAP + 1)
    spacing = spacing.at[0].set(GAP)
    blocks = LEN + spacing
    ending = jnp.cumsum(blocks, axis=1)
    return (ending - blocks).reshape(-1).astype(jnp.int32)


def place_ends(drawn, key, least, largest):
    longest = drawn.shape.index(max(drawn.shape))
    spots = []
    for shift in (0, 1):
        where = [jax.random.randint(jax.random.fold_in(key, axis), (), 0, length) for axis, length in enumerate(drawn.shape)]
        where[longest] = (where[longest] + shift) % drawn.shape[longest]
        spots.append(tuple(where))
    return drawn.at[spots[0]].set(least).at[spots[1]].set(largest)


def strengthened(values, stream_key, source, target, blocks, factor):
    def block_of(axis_at):
        return (jnp.arange(values.shape[axis_at]) // (values.shape[axis_at] // blocks)).reshape((-1,) + (1,) * (values.ndim - 1 - axis_at))

    first = jax.random.permutation(stream_key, blocks)[block_of(target)]
    far = (block_of(target) + blocks // 2) % blocks
    return jnp.where((block_of(source) == first) | (block_of(source) == far), factor * values, values)


def level_of(own_key, extent, shards, smallest, top_value):
    level, own = 1.0, jax.random.fold_in(own_key, 6)
    for position, blocks in shards:
        heights = jnp.exp(jax.random.uniform(jax.random.fold_in(own, position), (blocks,), jnp.float32, smallest / len(shards), top_value / len(shards)))
        level = level * jnp.repeat(heights, extent[position] // blocks).reshape([-1 if axis == position else 1 for axis in range(len(extent))])
    return level


def noise(stream_key, shape, spread, bound, pieces=(), kind=jnp.bfloat16):
    drawn = jax.random.normal(stream_key, shape, jnp.float32) * spread
    if len(pieces) > 0:
        drawn = level_of(stream_key, shape, pieces, -0.22, 0.18) * drawn
    return jnp.clip(drawn, min=-bound, max=bound).astype(kind)


def heavy_noise(own_key, shape, deviation, bound, cuts, heavy, kind=jnp.bfloat16):
    values = deviation * jax.random.normal(own_key, shape, jnp.float32)
    if cuts:
        values = values * level_of(own_key, shape, cuts, -0.22, 0.18)
    return jnp.clip(strengthened(values, jax.random.fold_in(own_key, 3), *heavy), -bound, bound).astype(kind)


def setup_inputs(seed: int = 0) -> dict:
    splits = jax.random.split(jax.random.key(seed), 11)
    return {
        "patches": noise(splits[0], (D, IMAGES * LEN), 1.0, 6.0, ((0, 8), (1, 128))),
        "lengths": place_ends(jax.random.randint(splits[1], (IMAGES,), 1, LEN + 1), jax.random.fold_in(splits[1], 1), 1, LEN).astype(jnp.int32),
        "slot_plan": draw_slot_plan(jax.random.fold_in(splits[10], 71), 0),
        "starts": draw_starts(jax.random.fold_in(splits[10], 71), 0),
        "text_rows": noise(splits[4], (D, SEQ), 1.0, 6.0, ((0, 8), (1, 128))),
        "cotangent": heavy_noise(splits[5], (D, SEQ), 1.0, 24.0, ((0, 8), (1, 128)), (1, 0, 128, 5.5)),
        "ln_gain": jnp.clip(1.0 + 0.15 * jax.random.normal(splits[6], (D,), jnp.float32), 0.25, 1.75),
        "ln_bias": noise(splits[7], (D,), 0.5, 3.0, (), jnp.float32),
        "w_qkv": noise(splits[8], (3, D, D), D ** -0.5, 0.15625, ((1, 8),)),
        "w_out": noise(splits[9], (D, D), D ** -0.5, 0.15625, ((0, 8),)),
    }


epsilon = 1e-06

def layer_norm(inputs_f, ln_gain, ln_bias):
    average = lax.optimization_barrier(jnp.mean(inputs_f, axis=-1, keepdims=True))
    centred = inputs_f - average
    variance = lax.optimization_barrier(jnp.mean(centred * centred, axis=-1, keepdims=True))
    return centred * lax.rsqrt(variance + epsilon) * ln_gain + ln_bias

def image_block(patch_rows, lengths, ln_gain, ln_bias, w_qkv, w_out):
    count = patch_rows.shape[0]
    flat_rows = patch_rows.reshape(count * LEN, D)
    normed = layer_norm(flat_rows.astype(jnp.float32), ln_gain, ln_bias).astype(jnp.bfloat16)
    shape_heads = (count, LEN, HEADS, HEAD_DIM)
    queries = jnp.dot(normed, w_qkv[0].T, preferred_element_type=jnp.float32).astype(jnp.bfloat16).reshape(shape_heads)
    key_rows = jnp.dot(normed, w_qkv[1].T, preferred_element_type=jnp.float32).astype(jnp.bfloat16).reshape(shape_heads)
    value_rows = jnp.dot(normed, w_qkv[2].T, preferred_element_type=jnp.float32).astype(jnp.bfloat16).reshape(shape_heads)
    scores = jnp.einsum('bqhe,bkhe->bhqk', queries.astype(jnp.float32), key_rows.astype(jnp.float32))
    scores = scores * (1.0 / math.sqrt(HEAD_DIM))
    offsets = jnp.arange(LEN, dtype=jnp.int32)
    key_live = offsets[None, :] < jnp.maximum(lengths, 1)[:, None]
    scores = jnp.where(key_live[:, None, None, :], scores, -1e+30)
    top = lax.optimization_barrier(jnp.max(scores, axis=-1, keepdims=True))
    raised = jnp.exp(scores - top)
    weights = (raised / lax.optimization_barrier(jnp.sum(raised, axis=-1, keepdims=True))).astype(jnp.bfloat16)
    context = jnp.einsum('bhqk,bkhe->bqhe', weights.astype(jnp.float32), value_rows.astype(jnp.float32)).astype(jnp.bfloat16)
    is_live = offsets[None, :] < lengths[:, None]
    context = jnp.where(is_live[:, :, None, None], context, jnp.zeros_like(context))
    context = context.reshape(count * LEN, D)
    width_part = D // N_TENSOR
    attended_f = jnp.zeros((count * LEN, D), jnp.float32)
    for shard in range(N_TENSOR):
        piece = jnp.dot(context[:, shard * width_part:(shard + 1) * width_part], w_out[shard * width_part:(shard + 1) * width_part], preferred_element_type=jnp.float32)
        piece = lax.optimization_barrier(piece.astype(jnp.bfloat16))
        attended_f = attended_f + piece.astype(jnp.float32)
    attended = attended_f.astype(jnp.bfloat16)
    merged = (flat_rows.astype(jnp.float32) + attended.astype(jnp.float32)).astype(jnp.bfloat16)
    return (merged.reshape(count, LEN, D), context)

def reference(patches, lengths, slot_plan, starts, text_rows, cotangent, ln_gain, ln_bias, w_qkv, w_out):
    groups = N_DP * N_PIPE
    image_all = patches.T.reshape(groups, IMG_DEV, LEN, D)
    length_all = lengths.reshape(groups, IMG_DEV)
    slot_all = slot_plan.reshape(groups, IMG_DEV)
    offsets = jnp.arange(LEN, dtype=jnp.int32)
    cot_seq = cotangent.T

    def one_group(grad_sum, inputs):
        group_id, patch_rows, group_len, group_slot = inputs
        merged, context = image_block(patch_rows, group_len, ln_gain, ln_bias, w_qkv, w_out)
        dp_index = group_id // N_PIPE
        pipe_index = group_id % N_PIPE
        owner_index = group_slot // CAP * N_PIPE + pipe_index
        place_index = dp_index * CAP + group_slot % CAP
        block_start = starts[(owner_index * SLOTS + place_index).astype(jnp.int32)]
        row_index = owner_index[:, None] * SEQ_DEV + block_start[:, None] + offsets[None, :]
        is_live = offsets[None, :] < group_len[:, None]
        row_index = jnp.where(is_live, row_index, SEQ).astype(jnp.int32)
        cot_rows = cot_seq[jnp.minimum(row_index, SEQ - 1).reshape(-1)]
        grad_sum = grad_sum + jnp.dot(context.T, cot_rows, preferred_element_type=jnp.float32)
        return (grad_sum, (merged, row_index))
    group_ids = jnp.arange(groups, dtype=jnp.int32)
    grad_sum, (merged_all, row_all) = lax.scan(one_group, jnp.zeros((D, D), jnp.float32), (group_ids, image_all, length_all, slot_all))
    features = text_rows.T.at[row_all.reshape(-1)].set(merged_all.reshape(-1, D), mode='drop').T
    return (features, grad_sum)
```

```python
import functools
import math

import jax
import jax.numpy as jnp
from jax import lax
from jax.experimental import pallas as pl
from jax.experimental.pallas import tpu as pltpu
from jax.sharding import PartitionSpec as P

HEAD_DIM = 80
LANES = 128
EPSILON = 1e-06
F32 = jnp.float32
BF16 = jnp.bfloat16
MESH = pl.DeviceIdType.MESH


def dot(a, b, ca=1, cb=0):
    return lax.dot_general(a, b, (((ca,), (cb,)), ((), ())), preferred_element_type=F32)


def iota(shape, dim):
    return lax.broadcasted_iota(jnp.int32, shape, dim)


def kernel(
    g,
    patches_hbm,
    text_hbm,
    cot_hbm,
    wqkv_hbm,
    wout_hbm,
    lengths_ref,
    slots_ref,
    starts_ref,
    gain_ref,
    bias_ref,
    features_ref,
    grad_ref,
    patches,
    text,
    cot,
    wqkv,
    wout,
    xfull,
    cfull,
    w_split,
    w_full,
    onehot,
    pick,
    gainb,
    biasb,
    cot_out,
    cot_in,
    cot_sel,
    merged_out,
    merged_in,
    grad_own,
    pair_out,
    pair_in,
    row_out,
    row_in,
    col_out,
    col_in,
    load_sem,
    xs_sem,
    xr_sem,
    cs_sem,
    cr_sem,
    a2a_send,
    a2a_recv,
    w_send,
    w_recv,
    pair_send,
    pair_recv,
    row_send,
    row_recv,
    col_send,
    col_recv,
):
    nx, nz, ny = g.nx, g.nz, g.ny
    ndp = nx * nz
    rows, width, chunks = g.rows, g.width, g.chunks
    cols = width * chunks
    length = g.length
    slots = ndp * length
    dp, y, c = lax.axis_index("dp"), lax.axis_index("tensor"), lax.axis_index("pipe")
    x, z = dp // nz, lax.rem(dp, nz)
    other = 1 - c

    loads = [
        pltpu.make_async_copy(a, b, load_sem.at[k])
        for k, (a, b) in enumerate(
            (
                (patches_hbm, patches),
                (cot_hbm, cot),
                (wout_hbm, wout),
                (wqkv_hbm, wqkv),
                (text_hbm, text),
            )
        )
    ]
    for load in loads:
        load.start()

    def plane_peer(k):
        return (
            lax.rem(x + k // nz, nx) * nz + lax.rem(z + lax.rem(k + nz // 2, nz), nz),
            y,
            c,
        )

    barrier = pltpu.get_barrier_semaphore()

    def greet(device):
        pl.semaphore_signal(barrier, inc=1, device_id=device, device_id_type=MESH)

    for k in range(1, ny):
        greet((dp, lax.rem(y + k, ny), c))
    greet((dp, y, other))

    def greet_plane(k, carry):
        greet(plane_peer(k))
        return carry

    lax.fori_loop(0, nz // 2, greet_plane, 0)
    lax.fori_loop(nz // 2 + 1, ndp, greet_plane, 0)
    per_t = ndp // ny
    per_x = ny // nx
    source_x = lax.rem(y // per_x + nx // 2, nx)
    source_y = dp // per_t

    def greet_source(k, carry):
        greet((source_x * nz + k, source_y, c))
        return carry

    lax.fori_loop(0, nz, greet_source, 0)
    pl.semaphore_wait(barrier, ny - 1 + 1 + ndp - 1 + nz)

    half = ny // 2
    limits = [(half, ny - 1 - half) if ch % 2 == 0 else (ny - 1 - half, half) for ch in range(chunks)]

    def hop(buf, ssem, rsem, way, step, ch):
        if way == 0:
            origin, peer = lax.rem(y + ny - step, ny), lax.rem(y + 1, ny)
        else:
            origin, peer = lax.rem(y + step, ny), lax.rem(y + ny - 1, ny)
        return pltpu.make_async_remote_copy(
            src_ref=buf.at[ch, origin],
            dst_ref=buf.at[ch, origin],
            send_sem=ssem.at[way, step, ch],
            recv_sem=rsem.at[way, step, ch],
            device_id=(dp, peer, c),
            device_id_type=MESH,
        )

    hop_x = functools.partial(hop, xfull, xs_sem, xr_sem)
    hop_c = functools.partial(hop, cfull, cs_sem, cr_sem)

    def open_ring(hops, ch):
        for way in range(2):
            if limits[ch][way] > 0:
                hops(way, 0, ch).start()

    def turn(hops, step, ch):
        for way in range(2):
            if step < limits[ch][way]:
                hops(way, step, ch).wait_recv()
                if step + 1 < limits[ch][way]:
                    hops(way, step + 1, ch).start()

    def close_ring(hops):
        for ch in range(chunks):
            for way in range(2):
                for step in range(limits[ch][way]):
                    hops(way, step, ch).wait_send()

    def exchange(send, recv, k):
        def start(n, carry):
            peer = plane_peer(n)
            pltpu.make_async_remote_copy(
                src_ref=send.at[peer[0]],
                dst_ref=recv.at[dp],
                send_sem=a2a_send.at[k],
                recv_sem=a2a_recv.at[k],
                device_id=peer,
                device_id_type=MESH,
            ).start()
            return carry

        lax.fori_loop(0, nz // 2, start, 0)
        lax.fori_loop(nz // 2 + 1, ndp, start, 0)
        recv[dp] = send[dp]

    def exchanged(send, recv, k):
        part = pl.ds(0, ndp - 1)
        pltpu.make_async_copy(recv.at[part], recv.at[part], a2a_recv.at[k]).wait()
        pltpu.make_async_copy(send.at[part], send.at[part], a2a_send.at[k]).wait()

    loads[0].wait()
    for ch in range(chunks):
        xfull[ch, y] = patches[:, ch * width : (ch + 1) * width]
        open_ring(hop_x, ch)

    place = iota((slots, ndp), 0) // length == iota((slots, ndp), 1)
    position = jnp.sum(
        jnp.where(place, starts_ref[...].astype(F32), 0.0), axis=1, keepdims=True
    ).astype(jnp.int32) + lax.rem(iota((slots, 1), 0), length)
    seq = g.seq
    onehot[...] = (iota((slots, seq), 1) == position).astype(F32).astype(BF16)
    loads[1].wait()
    each, room = g.each, LANES // per_t
    lined = iota((2 * LANES, rows), 0)
    rest = lax.rem(lined, LANES)
    column = (rest // room * 2 + lined // LANES) * each + lax.rem(rest, room)
    order = ((lax.rem(rest, room) < each) & (column == iota((2 * LANES, rows), 1))).astype(F32).astype(BF16)
    cot_lined = dot(order, cot[...]).astype(BF16)
    pair = [
        dot(onehot[...], cot_lined[k * LANES : (k + 1) * LANES], 1, 1).reshape(ndp, length, LANES)
        for k in range(2)
    ]
    cot_out[...] = jnp.concatenate(pair, axis=1).astype(BF16)
    exchange(cot_out, cot_in, 0)

    for ch in range(chunks):
        turn(hop_x, 0, ch)
    loads[2].wait()
    w_split[...] = wout[...].T.reshape(w_split.shape)
    for ch in range(chunks):
        turn(hop_x, 1, ch) if ny > 2 else None
    gainb[...] = jnp.broadcast_to(gain_ref[...], (width, rows * ny)).T
    biasb[...] = jnp.broadcast_to(bias_ref[...], (width, rows * ny)).T
    images = cols // length
    spread = (iota((images, cols), 1) // length == iota((images, cols), 0)).astype(F32).astype(BF16)

    def per_column(ref):
        values = jnp.broadcast_to(ref[...].astype(F32), (8, images)).astype(BF16)
        return dot(values, spread)[0:1].astype(jnp.int32)

    live_len = per_column(lengths_ref)
    within = lax.rem(iota((1, cols), 1), length)
    target = per_column(slots_ref) * length + within
    live = within < live_len
    pick[...] = (iota((slots, cols), 0) == target).astype(F32).astype(BF16)
    for step in range(2, half - 1):
        for ch in range(chunks):
            turn(hop_x, step, ch)

    def w_copy(k):
        peer = lax.rem(y + k, ny)
        return pltpu.make_async_remote_copy(
            src_ref=w_split.at[peer, c],
            dst_ref=w_full.at[c, y],
            send_sem=w_send.at[0],
            recv_sem=w_recv.at[0],
            device_id=(dp, peer, c),
            device_id_type=MESH,
        )

    for k in sorted(range(1, ny), key=lambda k: -min(k, ny - k)):
        w_copy(k).start()
    w_full[c, y] = w_split[y, c]
    w_pair = pltpu.make_async_remote_copy(
        src_ref=w_full.at[c],
        dst_ref=w_full.at[c],
        send_sem=w_send.at[1],
        recv_sem=w_recv.at[1],
        device_id=(dp, y, other),
        device_id_type=MESH,
    )

    loads[3].wait()
    key_row, query_col = iota((width, width), 0), iota((width, width), 1)
    same = key_row // length == query_col // length
    for ch in range(chunks):
        if ny > 2:
            turn(hop_x, half - 1, ch)
        here = slice(ch * width, (ch + 1) * width)
        inputs = xfull[ch].reshape(ny * rows, width).astype(F32)
        centred = inputs - jnp.mean(inputs, axis=0, keepdims=True)
        variance = jnp.mean(centred * centred, axis=0, keepdims=True)
        normed = (centred * lax.rsqrt(variance + EPSILON) * gainb[...] + biasb[...]).astype(BF16)
        queries, keys, values = (dot(wqkv[k], normed).astype(BF16) for k in range(3))
        mask = same & (lax.rem(key_row, length) < live_len[:, here])
        contexts = []
        for head in range(rows // HEAD_DIM):
            part = slice(head * HEAD_DIM, (head + 1) * HEAD_DIM)
            scores = dot(keys[part], queries[part], 0, 0) * (1.0 / math.sqrt(HEAD_DIM))
            scores = jnp.where(mask, scores, -1e30)
            raised = jnp.exp(scores - jnp.max(scores, axis=0, keepdims=True))
            weights = (raised / jnp.sum(raised, axis=0, keepdims=True)).astype(BF16)
            contexts.append(dot(values[part], weights))
        context = jnp.concatenate(contexts, axis=0)
        cfull[ch, y] = jnp.where(live[:, here], context, 0.0).astype(BF16)
        open_ring(hop_c, ch)
    close_ring(hop_x)

    exchanged(cot_out, cot_in, 0)
    arrived = cot_in[...].astype(F32)
    for k in range(2):
        block = arrived[:, k * length : (k + 1) * length].reshape(slots, LANES).astype(BF16)
        cot_sel[k] = dot(block, pick[...], 0, 0).astype(BF16)

    for ch in range(chunks):
        turn(hop_c, 0, ch)
    part = pl.ds(0, ny - 1)
    pltpu.make_async_copy(w_full.at[c, part], w_full.at[c, part], w_recv.at[0]).wait()
    pltpu.make_async_copy(w_full.at[c, part], w_full.at[c, part], w_send.at[0]).wait()
    w_pair.start()
    for step in range(1, half):
        for ch in range(chunks):
            turn(hop_c, step, ch)
    w_pair.wait()

    pieces = []
    for ch in range(chunks):
        here = slice(ch * width, (ch + 1) * width)
        attended = jnp.zeros((rows, width), F32)
        for t in range(ny):
            block = jnp.concatenate([w_full[0, t], w_full[1, t]], axis=0)
            attended += dot(block, cfull[ch, t]).astype(BF16).astype(F32)
        merged = patches[:, here].astype(F32) + attended.astype(BF16).astype(F32)
        alive = jnp.where(live[:, here] & (iota((2 * LANES - rows, width), 0) == 0), 1.0, 0.0)
        pieces.append(jnp.concatenate([merged, alive], axis=0).astype(BF16))
    merged = jnp.concatenate(pieces, axis=1)
    pair = [
        dot(pick[...], merged[k * LANES : (k + 1) * LANES], 1, 1).reshape(ndp, length, LANES)
        for k in range(2)
    ]
    merged_out[...] = jnp.concatenate(pair, axis=1).astype(BF16)
    exchange(merged_out, merged_in, 1)

    def term(k):
        total = jnp.zeros((ny * rows, LANES), F32)
        for ch in range(chunks):
            block = cot_sel[k, :, ch * width : (ch + 1) * width]
            total += dot(cfull[ch].reshape(ny * rows, width), block, 1, 1)
        return total

    pair_out[...] = term(other).astype(pair_out.dtype)
    pair_copy = pltpu.make_async_remote_copy(
        src_ref=pair_out,
        dst_ref=pair_in,
        send_sem=pair_send,
        recv_sem=pair_recv,
        device_id=(dp, y, other),
        device_id_type=MESH,
    )
    pair_copy.start()
    grad_own[...] = term(c).reshape(grad_own.shape)
    pair_copy.wait()
    grad_own[...] += pair_in[...].astype(F32).reshape(grad_own.shape)
    row_out[...] = grad_own[...].astype(BF16)
    row_copies = []
    for k in range(1, nx):
        peer = lax.rem(x + k, nx)
        row_copies.append(
            pltpu.make_async_remote_copy(
                src_ref=row_out.at[lax.rem(peer + nx // 2, nx)],
                dst_ref=row_in.at[k - 1],
                send_sem=row_send.at[k - 1],
                recv_sem=row_recv.at[k - 1],
                device_id=(peer * nz + z, y, c),
                device_id_type=MESH,
            )
        )
        row_copies[-1].start()
    share = lax.rem(x + nx // 2, nx)
    total = grad_own[share]
    for k, copy in enumerate(row_copies):
        copy.wait()
        total += row_in[k].astype(F32)
    for b in range(per_x):
        turned = total[b * rows : (b + 1) * rows].T
        col_out[b] = turned.reshape(per_t, room, rows).astype(BF16)

    def send_column(k, carry):
        b, target = k // per_t, lax.rem(k, per_t)
        pltpu.make_async_remote_copy(
            src_ref=col_out.at[b, target],
            dst_ref=col_in.at[z],
            send_sem=col_send,
            recv_sem=col_recv,
            device_id=(y * per_t + target, share * per_x + b, c),
            device_id_type=MESH,
        ).start()
        return carry

    lax.fori_loop(0, per_x * per_t, send_column, 0)
    close_ring(hop_c)

    exchanged(merged_out, merged_in, 1)
    loads[4].wait()
    arrived = merged_in[...].astype(F32)
    first = arrived[:, :length].reshape(slots, LANES).T.astype(BF16)
    second = arrived[:, length:].reshape(slots, LANES).T.astype(BF16)
    over = rows - LANES
    wide = g.seq_block
    for k in range(seq // wide):
        here = slice(k * wide, (k + 1) * wide)
        spots = onehot[:, here]
        upper, lower = dot(first, spots), dot(second, spots)
        covered = lower[over : over + 1] > 0.5
        placed = jnp.concatenate([upper, lower[:over]], axis=0).astype(BF16)
        features_ref[:, here] = jnp.where(covered, placed, text[:, here])

    pltpu.make_async_copy(col_in, col_in, col_recv).wait()
    pltpu.make_async_copy(col_out, col_out, col_send).wait()
    total = jnp.sum(col_in[...].astype(F32), axis=0)
    grad_ref[...] = total.T[:, :each]


class Geometry:
    def __init__(self, nx, nz, ny, rows, cols, images, seq):
        self.nx, self.nz, self.ny, self.rows = nx, nz, ny, rows
        self.length = cols // images
        self.chunks = 3
        self.width = cols // self.chunks
        self.seq = seq
        self.seq_block = 256 if seq % 256 == 0 else seq
        self.each = rows * ny // (nx * nz * 2)


def shards(nx, patches, lengths, slot_plan, starts, text_rows, cotangent, ln_gain, ln_bias, w_qkv, w_out):
    ndp, ny = lax.axis_size("dp"), lax.axis_size("tensor")
    rows, cols = patches.shape
    d = w_out.shape[1]
    seq = text_rows.shape[1]
    g = Geometry(nx, ndp // nx, ny, rows, cols, lengths.shape[0], seq)
    slots = ndp * g.length
    per_t, per_x, room = ndp // ny, ny // nx, LANES // (ndp // ny)
    half = max(ny // 2, 1)
    hbm, vmem = pl.BlockSpec(memory_space=pl.ANY), pl.BlockSpec(memory_space=pltpu.VMEM)
    dma = pltpu.SemaphoreType.DMA
    ring = (g.chunks, ny, rows, g.width)
    packets = (ndp, 2 * g.length, LANES)
    scratch = [
        pltpu.VMEM(patches.shape, BF16),
        pltpu.VMEM(text_rows.shape, BF16),
        pltpu.VMEM(cotangent.shape, BF16),
        pltpu.VMEM(w_qkv.shape, BF16),
        pltpu.VMEM(w_out.shape, BF16),
        pltpu.VMEM(ring, BF16),
        pltpu.VMEM(ring, BF16),
        pltpu.VMEM((ny, 2, rows // 2, rows), BF16),
        pltpu.VMEM((2, ny, rows // 2, rows), BF16),
        pltpu.VMEM((slots, seq), BF16),
        pltpu.VMEM((slots, cols), BF16),
        pltpu.VMEM((d, g.width), F32),
        pltpu.VMEM((d, g.width), F32),
        pltpu.VMEM(packets, BF16),
        pltpu.VMEM(packets, BF16),
        pltpu.VMEM((2, LANES, cols), BF16),
        pltpu.VMEM(packets, BF16),
        pltpu.VMEM(packets, BF16),
        pltpu.VMEM((nx, d // nx, LANES), F32),
        pltpu.VMEM((d, LANES), F32),
        pltpu.VMEM((d, LANES), F32),
        pltpu.VMEM((nx, d // nx, LANES), BF16),
        pltpu.VMEM((nx - 1, d // nx, LANES), BF16),
        pltpu.VMEM((per_x, per_t, room, rows), BF16),
        pltpu.VMEM((g.nz, room, rows), BF16),
        dma((5,)),
        dma((2, half, g.chunks)),
        dma((2, half, g.chunks)),
        dma((2, half, g.chunks)),
        dma((2, half, g.chunks)),
        dma((2,)),
        dma((2,)),
        dma((2,)),
        dma((2,)),
        dma,
        dma,
        dma((nx - 1,)),
        dma((nx - 1,)),
        dma,
        dma,
    ]
    return pl.pallas_call(
        functools.partial(kernel, g),
        out_shape=(
            jax.ShapeDtypeStruct(text_rows.shape, BF16),
            jax.ShapeDtypeStruct((rows, g.each), F32),
        ),
        in_specs=[hbm] * 5 + [vmem] * 5,
        out_specs=(vmem, vmem),
        scratch_shapes=scratch,
        compiler_params=pltpu.CompilerParams(collective_id=0, has_side_effects=True, vmem_limit_bytes=48 << 20),
    )(
        patches,
        text_rows,
        cotangent,
        w_qkv,
        w_out,
        lengths.reshape(1, -1),
        slot_plan.reshape(1, -1),
        starts.reshape(1, -1),
        ln_gain.reshape(1, -1),
        ln_bias.reshape(1, -1),
    )


def solution(mesh, nx=4):
    groups = ("dp", "pipe")
    in_specs = (
        P("tensor", groups),
        P(groups),
        P(groups),
        P(groups),
        P("tensor", groups),
        P("tensor", groups),
        P(),
        P(),
        P(None, "tensor", None),
        P("tensor", None),
    )
    out_specs = (P("tensor", groups), P("tensor", groups))
    return jax.shard_map(
        functools.partial(shards, nx), mesh=mesh, in_specs=in_specs, out_specs=out_specs, check_vma=False
    )
```

```python
import functools
import math

import jax
import jax.numpy as jnp
from jax import lax
from jax.experimental import pallas as pl
from jax.experimental.pallas import tpu as pltpu
from jax.sharding import PartitionSpec as P

HEAD_DIM = 80
LANES = 128
EPSILON = 1e-06
F32 = jnp.float32
BF16 = jnp.bfloat16
MESH = pl.DeviceIdType.MESH


def dot(a, b, ca=1, cb=0):
    return lax.dot_general(a, b, (((ca,), (cb,)), ((), ())), preferred_element_type=F32)


def iota(shape, dim):
    return lax.broadcasted_iota(jnp.int32, shape, dim)


def kernel(
    g,
    patches_hbm,
    text_hbm,
    cot_hbm,
    wqkv_hbm,
    wout_hbm,
    lengths_hbm,
    slots_hbm,
    starts_hbm,
    gain_hbm,
    bias_hbm,
    features_ref,
    grad_ref,
    patches,
    text,
    cot,
    wqkv,
    wout,
    lengths_ref,
    slots_ref,
    starts_ref,
    gain_ref,
    bias_ref,
    xfull,
    cfull,
    w_split,
    w_full,
    onehot,
    pick,
    gainb,
    biasb,
    cot_out,
    cot_in,
    cot_sel,
    merged_out,
    merged_in,
    attended,
    grad_own,
    pair_out,
    pair_in,
    row_out,
    row_in,
    col_out,
    col_in,
    near_sem,
    load_sem,
    xs_sem,
    xr_sem,
    cs_sem,
    cr_sem,
    a2a_send,
    a2a_recv,
    w_send,
    w_recv,
    pair_send,
    pair_recv,
    row_send,
    row_recv,
    col_send,
    col_recv,
):
    nx, nz, ny = g.nx, g.nz, g.ny
    ndp = nx * nz
    rows, width, chunks = g.rows, g.width, g.chunks
    cols = width * chunks
    length = g.length
    slots = ndp * length
    dp, y, c = lax.axis_index("dp"), lax.axis_index("tensor"), lax.axis_index("pipe")
    x, z = dp // nz, lax.rem(dp, nz)
    other = 1 - c

    loads = [
        pltpu.make_async_copy(a, b, load_sem.at[k])
        for k, (a, b) in enumerate(
            (
                (patches_hbm, patches),
                (cot_hbm, cot),
                (wout_hbm, wout),
                (wqkv_hbm, wqkv),
                (text_hbm, text),
                (lengths_hbm, lengths_ref.at[0]),
                (slots_hbm, slots_ref.at[0]),
                (starts_hbm, starts_ref.at[0]),
                (gain_hbm, gain_ref.at[0]),
                (bias_hbm, bias_ref.at[0]),
            )
        )
    ]
    for load in loads:
        load.start()

    def plane_peer(k):
        return (
            lax.rem(x + k // nz, nx) * nz + lax.rem(z + lax.rem(k + nz // 2, nz), nz),
            y,
            c,
        )

    phase = Phase()
    phase('greet')
    barrier = pltpu.get_barrier_semaphore()

    def signal(sem, device):
        pl.semaphore_signal(sem, inc=1, device_id=device, device_id_type=MESH)

    def place_at(dx, dz):
        return (lax.rem(x + dx, nx) * nz + lax.rem(z + dz, nz), y, c)

    signal(barrier, (dp, y, other))
    for way in (1, -1):
        signal(barrier, (dp, lax.rem(y + ny + way, ny), c))
        signal(barrier, place_at(0, nz + way))
        signal(barrier, place_at(nx + way, 0))
    phase('barrier_wait')
    pl.semaphore_wait(barrier, 7)

    rounds = []
    for count, axis in ((nz, 1), (nx, 0)):
        reach = 1
        while reach < count // 2:
            step = [(count + reach), (count - reach)]
            rounds.append([(0, r) if axis else (r, 0) for r in step])
            reach *= 2
    rounds.append([(r, 0) for r in range(1, nx)])

    def knock(n):
        for dx, dz in rounds[n]:
            signal(near_sem.at[n], place_at(dx, dz))

    def hear(n):
        pl.semaphore_wait(near_sem.at[n], len(rounds[n]))

    half = ny // 2
    parts = 2
    tall = rows // parts
    units = [(ch, h) for ch in range(chunks) for h in range(parts)]
    limits = {u: (half, ny - 1 - half) if n % 2 == 0 else (ny - 1 - half, half) for n, u in enumerate(units)}

    def hop(buf, ssem, rsem, way, step, unit):
        ch, h = unit
        if way == 0:
            origin, peer = lax.rem(y + ny - step, ny), lax.rem(y + 1, ny)
        else:
            origin, peer = lax.rem(y + step, ny), lax.rem(y + ny - 1, ny)
        piece = buf.at[ch, origin, pl.ds(h * tall, tall)]
        n = ch * parts + h
        return pltpu.make_async_remote_copy(
            src_ref=piece,
            dst_ref=piece,
            send_sem=ssem.at[way, step, n],
            recv_sem=rsem.at[way, step, n],
            device_id=(dp, peer, c),
            device_id_type=MESH,
        )

    hop_x = functools.partial(hop, xfull, xs_sem, xr_sem)
    hop_c = functools.partial(hop, cfull, cs_sem, cr_sem)

    def open_ring(hops, ch):
        for h in range(parts):
            for way in range(2):
                if limits[ch, h][way] > 0:
                    hops(way, 0, (ch, h)).start()

    def turn(hops, step, ch):
        for h in range(parts):
            for way in range(2):
                if step < limits[ch, h][way]:
                    hops(way, step, (ch, h)).wait_recv()
                    if step + 1 < limits[ch, h][way]:
                        hops(way, step + 1, (ch, h)).start()

    def close_ring(hops):
        for unit in units:
            for way in range(2):
                for step in range(limits[unit][way]):
                    hops(way, step, unit).wait_send()

    def exchange(send, recv, k, low, high):
        count = high - low
        if count == 0:
            return

        def start(n, carry):
            peer = place_at(n // count, low + lax.rem(n, count))
            pltpu.make_async_remote_copy(
                src_ref=send.at[peer[0]],
                dst_ref=recv.at[dp],
                send_sem=a2a_send.at[k],
                recv_sem=a2a_recv.at[k],
                device_id=peer,
                device_id_type=MESH,
            ).start()
            return carry

        lax.fori_loop(0 if low % nz else 1, nx * count, start, 0)

    def exchanged(send, recv, k):
        part = pl.ds(0, ndp - 1)
        pltpu.make_async_copy(recv.at[part], recv.at[part], a2a_recv.at[k]).wait()
        pltpu.make_async_copy(send.at[part], send.at[part], a2a_send.at[k]).wait()

    phase('open_x')
    loads[0].wait()
    for ch in range(chunks):
        xfull[ch, y] = patches[:, ch * width : (ch + 1) * width]
        open_ring(hop_x, ch)
    z_rounds = 0
    while 2 ** (z_rounds + 1) <= nz // 2:
        z_rounds += 1
    last_round = len(rounds) - 1
    if z_rounds:
        knock(0)
    for n in range(z_rounds, last_round):
        knock(n)

    phase('cot_out')
    for load in loads[5:]:
        load.wait()
    place = iota((slots, ndp), 0) // length == iota((slots, ndp), 1)
    position = jnp.sum(
        jnp.where(place, starts_ref[...].astype(F32), 0.0), axis=1, keepdims=True
    ).astype(jnp.int32) + lax.rem(iota((slots, 1), 0), length)
    seq = g.seq
    onehot[...] = (iota((slots, seq), 1) == position).astype(F32).astype(BF16)
    loads[1].wait()
    each, room = g.each, LANES // g.per_t
    lined = iota((2 * LANES, rows), 0)
    rest = lax.rem(lined, LANES)
    column = (rest // room * 2 + lined // LANES) * each + lax.rem(rest, room)
    order = ((lax.rem(rest, room) < each) & (column == iota((2 * LANES, rows), 1))).astype(F32).astype(BF16)
    cot_lined = dot(order, cot[...]).astype(BF16)
    pair = [
        dot(onehot[...], cot_lined[k * LANES : (k + 1) * LANES], 1, 1).reshape(ndp, length, LANES)
        for k in range(2)
    ]
    cot_out[...] = jnp.concatenate(pair, axis=1).astype(BF16)
    cot_in[dp] = cot_out[dp]

    images = cols // length
    spread = (iota((images, cols), 1) // length == iota((images, cols), 0)).astype(F32).astype(BF16)

    def per_column(ref):
        values = jnp.broadcast_to(ref[...].astype(F32), (8, images)).astype(BF16)
        return dot(values, spread)[0:1].astype(jnp.int32)

    live_len = per_column(lengths_ref)
    within = lax.rem(iota((1, cols), 1), length)
    target = per_column(slots_ref) * length + within
    live = within < live_len

    def turn_weights():
        loads[2].wait()
        w_split[...] = wout[...].T.reshape(w_split.shape)
        w_full[c, y] = w_split[y, c]

    def spread_norm():
        gainb[...] = jnp.broadcast_to(gain_ref[...], (width, rows * ny)).T
        biasb[...] = jnp.broadcast_to(bias_ref[...], (width, rows * ny)).T

    def build_pick():
        pick[...] = (iota((slots, cols), 0) == target).astype(F32).astype(BF16)

    tasks = [turn_weights, spread_norm, build_pick]
    heard = 0

    def next_round():
        nonlocal heard
        if heard < z_rounds:
            hear(heard)
            heard += 1
            if heard < z_rounds:
                knock(heard)
        if heard == z_rounds:
            for n in range(z_rounds, last_round):
                hear(n)
            knock(last_round)
            heard += 1

    for step in range(half - 1):
        phase('turn_x%d' % step)
        for ch in range(chunks):
            turn(hop_x, step, ch)
        next_round()
        if tasks:
            tasks.pop(0)()
    phase('rounds')
    for task in tasks:
        task()
    while heard <= z_rounds:
        next_round()

    def w_copy(k):
        peer = lax.rem(y + k, ny)
        return pltpu.make_async_remote_copy(
            src_ref=w_split.at[peer, c],
            dst_ref=w_full.at[c, y],
            send_sem=w_send.at[0],
            recv_sem=w_recv.at[0],
            device_id=(dp, peer, c),
            device_id_type=MESH,
        )

    far_first = sorted(range(1, ny), key=lambda k: -min(k, ny - k))
    for k in far_first:
        if k != half:
            w_copy(k).start()
    w_pair = pltpu.make_async_remote_copy(
        src_ref=w_full.at[c],
        dst_ref=w_full.at[c],
        send_sem=w_send.at[1],
        recv_sem=w_recv.at[1],
        device_id=(dp, y, other),
        device_id_type=MESH,
    )
    hear(last_round)
    phase('cot_send')
    near = max(nz // 4, 1)
    exchange(cot_out, cot_in, 0, near, nz - near + 1)
    exchange(cot_out, cot_in, 0, nz - near + 1, nz)
    exchange(cot_out, cot_in, 0, 0, near)

    loads[3].wait()
    key_row, query_col = iota((width, width), 0), iota((width, width), 1)
    same = key_row // length == query_col // length
    for ch in range(chunks):
        phase('turn_x_last_%d' % ch)
        turn(hop_x, half - 1, ch)
        if ch == 0:
            w_copy(half).start()
        phase('attention_%d' % ch)
        here = slice(ch * width, (ch + 1) * width)
        inputs = xfull[ch].reshape(ny * rows, width).astype(F32)
        centred = inputs - jnp.mean(inputs, axis=0, keepdims=True)
        variance = jnp.mean(centred * centred, axis=0, keepdims=True)
        normed = (centred * lax.rsqrt(variance + EPSILON) * gainb[...] + biasb[...]).astype(BF16)
        queries, keys, values = (dot(wqkv[k], normed).astype(BF16) for k in range(3))
        mask = same & (lax.rem(key_row, length) < live_len[:, here])
        contexts = []
        for head in range(rows // HEAD_DIM):
            part = slice(head * HEAD_DIM, (head + 1) * HEAD_DIM)
            scores = dot(keys[part], queries[part], 0, 0) * (1.0 / math.sqrt(HEAD_DIM))
            scores = jnp.where(mask, scores, -1e30)
            raised = jnp.exp(scores - jnp.max(scores, axis=0, keepdims=True))
            weights = (raised / jnp.sum(raised, axis=0, keepdims=True)).astype(BF16)
            contexts.append(dot(values[part], weights))
        context = jnp.concatenate(contexts, axis=0)
        cfull[ch, y] = jnp.where(live[:, here], context, 0.0).astype(BF16)
        open_ring(hop_c, ch)
    phase('close_x')
    close_ring(hop_x)

    arrivals = [0]
    for away in range(1, half + 1):
        arrivals += [away, ny - away] if away < half else [away]
    per_x = g.per_x
    shares = [arrivals[k * per_x : (k + 1) * per_x] for k in range(nx)]
    ready = [max(max(min(a, ny - a) for a in share) - 1, 0) for share in shares]
    home_x = y * g.per_t // nz
    mine = lax.rem(x + nx - home_x + nx // 2, nx)

    def block_at(away):
        return lax.rem(y + away, ny)

    def project(away):
        at = block_at(away)
        weights = jnp.concatenate([w_full[0, at], w_full[1, at]], axis=0)
        for ch in range(chunks):
            piece = dot(weights, cfull[ch, at]).astype(BF16).astype(F32)
            attended[ch] = piece if away == 0 else attended[ch] + piece

    def pair_copy(k):
        return pltpu.make_async_remote_copy(
            src_ref=pair_out.at[k],
            dst_ref=pair_in.at[k],
            send_sem=pair_send.at[k],
            recv_sem=pair_recv.at[k],
            device_id=(dp, y, other),
            device_id_type=MESH,
        )

    def term(k, side):
        blocks = []
        for away in shares[k]:
            total = jnp.zeros((rows, LANES), F32)
            for ch in range(chunks):
                block = cot_sel[side, :, ch * width : (ch + 1) * width]
                total += dot(cfull[ch, block_at(away)], block, 1, 1)
            blocks.append(total)
        return jnp.concatenate(blocks, axis=0)

    def first_stage(k):
        pair_out[k] = term(k, other)
        pair_copy(k).start()
        grad_own[k] = term(k, c)

    def row_copy(k):
        peer = lax.rem(home_x + k + nx - nx // 2, nx)
        slot = lax.rem(peer - x + nx + nx - 1, nx)
        return pltpu.make_async_remote_copy(
            src_ref=row_out.at[k],
            dst_ref=row_in.at[slot],
            send_sem=row_send.at[k],
            recv_sem=row_recv.at[slot],
            device_id=(peer * nz + z, y, c),
            device_id_type=MESH,
        )

    def second_stage(k):
        pair_copy(k).wait()
        total = grad_own[k] + pair_in[k]
        grad_own[k] = total
        row_out[k] = total.astype(BF16)

        @pl.when(mine != k)
        def _():
            row_copy(k).start()

    def column_copy(b, target, away):
        return pltpu.make_async_remote_copy(
            src_ref=col_out.at[b, target],
            dst_ref=col_in.at[z],
            send_sem=col_send,
            recv_sem=col_recv,
            device_id=(y * g.per_t + target, block_at(away), c),
            device_id_type=MESH,
        )

    over = rows - LANES

    def third_stage(k):
        @pl.when(mine == k)
        def _():
            total = grad_own[k]
            for slot in range(nx - 1):
                arrived = pltpu.make_async_copy(row_in.at[slot], row_in.at[slot], row_recv.at[slot])
                arrived.wait()
                total += row_in[slot].astype(F32)
            for b, away in enumerate(shares[k]):
                turned = total[b * rows : (b + 1) * rows].T.reshape(g.per_t, room, rows)
                tail = turned[:, :each, LANES:]
                spare = jnp.zeros((g.per_t, each // 2, LANES - 2 * over), F32)
                tail = jnp.concatenate([tail[:, : each // 2], tail[:, each // 2 :], spare], axis=2)
                spare = jnp.zeros((g.per_t, room - each - each // 2, LANES), F32)
                packed = jnp.concatenate([turned[:, :each, :LANES], tail, spare], axis=1)
                col_out[b] = packed.astype(BF16)

                def send(target, carry, b=b, away=away):
                    column_copy(b, target, away).start()
                    return carry

                lax.fori_loop(0, g.per_t, send, 0)

    def select_cotangent():
        exchanged(cot_out, cot_in, 0)
        arrived = cot_in[...].astype(F32)
        for k in range(2):
            block = arrived[:, k * length : (k + 1) * length].reshape(slots, LANES).astype(BF16)
            cot_sel[k] = dot(block, pick[...], 0, 0).astype(BF16)

    begun, paired, ended, projected = 0, 0, 0, 0
    working = min(1, half - 1)
    for step in range(half):
        phase('turn_c%d' % step)
        for ch in range(chunks):
            turn(hop_c, step, ch)
        phase('work_c%d' % step)
        if step == 0:
            part = pl.ds(0, ny - 1)
            pltpu.make_async_copy(w_full.at[c, part], w_full.at[c, part], w_recv.at[0]).wait()
            pltpu.make_async_copy(w_full.at[c, part], w_full.at[c, part], w_send.at[0]).wait()
            w_pair.start()
        if step == working:
            phase('cot_wait')
            w_pair.wait()
            select_cotangent()
            phase('work_c%d' % step)
        if step < working:
            continue
        fresh = [k for k in range(begun, nx) if ready[k] <= step]
        for k in fresh:
            first_stage(k)
        while projected < ny and min(arrivals[projected], ny - arrivals[projected]) <= step + 1:
            project(arrivals[projected])
            projected += 1
        before = paired
        for k in range(paired, begun):
            second_stage(k)
            paired += 1
        for k in range(ended, before):
            third_stage(k)
            ended += 1
        begun += len(fresh)
        if step == half - 1:
            before = paired if paired < nx - 1 else nx - 2
            for k in range(ended, min(before, 2)):
                third_stage(k)
                ended += 1

    phase('merged_out')
    pieces = []
    for ch in range(chunks):
        here = slice(ch * width, (ch + 1) * width)
        merged = patches[:, here].astype(F32) + attended[ch].astype(BF16).astype(F32)
        alive = jnp.where(live[:, here] & (iota((2 * LANES - rows, width), 0) == 0), 1.0, 0.0)
        pieces.append(jnp.concatenate([merged, alive], axis=0).astype(BF16))
    merged = jnp.concatenate(pieces, axis=1)
    pair = [
        dot(pick[...], merged[k * LANES : (k + 1) * LANES], 1, 1).reshape(ndp, length, LANES)
        for k in range(2)
    ]
    merged_out[...] = jnp.concatenate(pair, axis=1).astype(BF16)
    merged_in[dp] = merged_out[dp]
    phase('pair_last')
    for k in range(paired, nx):
        second_stage(k)
    phase('merged_send')
    exchange(merged_out, merged_in, 1, near, nz - near + 1)
    phase('third')
    for k in range(ended, nx):
        third_stage(k)
    phase('merged_send2')
    exchange(merged_out, merged_in, 1, nz - near + 1, nz)
    exchange(merged_out, merged_in, 1, 0, near)
    close_ring(hop_c)
    for k in range(nx):
        @pl.when(mine != k)
        def _(k=k):
            row_copy(k).wait_send()

    phase('merged_wait')
    exchanged(merged_out, merged_in, 1)
    phase('place')
    loads[4].wait()
    arrived = merged_in[...].astype(F32)
    first = arrived[:, :length].reshape(slots, LANES).T.astype(BF16)
    second = arrived[:, length:].reshape(slots, LANES).T.astype(BF16)
    wide = g.seq_block
    for k in range(seq // wide):
        here = slice(k * wide, (k + 1) * wide)
        spots = onehot[:, here]
        upper, lower = dot(first, spots), dot(second, spots)
        covered = lower[over : over + 1] > 0.5
        placed = jnp.concatenate([upper, lower[:over]], axis=0).astype(BF16)
        features_ref[:, here] = jnp.where(covered, placed, text[:, here])

    phase('col_wait')
    pltpu.make_async_copy(col_in, col_in, col_recv).wait()
    pltpu.make_async_copy(col_out, col_out, col_send).wait()
    phase('finish')
    total = jnp.sum(col_in[...].astype(F32), axis=0)
    tail = total[each : each + each // 2]
    tail = jnp.concatenate([tail[:, :over], tail[:, over : 2 * over]], axis=0)
    grad_ref[...] = jnp.concatenate([total[:each], tail], axis=1)
    phase(None)


class Phase:
    scope = None

    def __call__(self, name):
        if self.scope is not None:
            self.scope.__exit__(None, None, None)
        self.scope = jax.named_scope(name) if name else None
        if name:
            self.scope.__enter__()


class Geometry:
    def __init__(self, nx, nz, ny, rows, cols, images, seq):
        self.nx, self.nz, self.ny, self.rows = nx, nz, ny, rows
        self.length = cols // images
        self.chunks = 3
        self.width = cols // self.chunks
        self.seq = seq
        self.seq_block = 256 if seq % 256 == 0 else seq
        self.per_t, self.per_x = nx * nz // ny, ny // nx
        self.each = rows * ny // (nx * nz * 2)


def shards(nx, patches, lengths, slot_plan, starts, text_rows, cotangent, ln_gain, ln_bias, w_qkv, w_out):
    ndp, ny = lax.axis_size("dp"), lax.axis_size("tensor")
    rows, cols = patches.shape
    d = w_out.shape[1]
    seq = text_rows.shape[1]
    g = Geometry(nx, ndp // nx, ny, rows, cols, lengths.shape[0], seq)
    slots = ndp * g.length
    room = LANES // g.per_t
    half = max(ny // 2, 1)
    hbm, vmem = pl.BlockSpec(memory_space=pl.ANY), pl.BlockSpec(memory_space=pltpu.VMEM)
    dma = pltpu.SemaphoreType.DMA
    ring = (g.chunks, ny, rows, g.width)
    packets = (ndp, 2 * g.length, LANES)
    scratch = [
        pltpu.VMEM(patches.shape, BF16),
        pltpu.VMEM(text_rows.shape, BF16),
        pltpu.VMEM(cotangent.shape, BF16),
        pltpu.VMEM(w_qkv.shape, BF16),
        pltpu.VMEM(w_out.shape, BF16),
        pltpu.VMEM((1,) + lengths.shape, jnp.int32),
        pltpu.VMEM((1,) + slot_plan.shape, jnp.int32),
        pltpu.VMEM((1,) + starts.shape, jnp.int32),
        pltpu.VMEM((1,) + ln_gain.shape, F32),
        pltpu.VMEM((1,) + ln_bias.shape, F32),
        pltpu.VMEM(ring, BF16),
        pltpu.VMEM(ring, BF16),
        pltpu.VMEM((ny, 2, rows // 2, rows), BF16),
        pltpu.VMEM((2, ny, rows // 2, rows), BF16),
        pltpu.VMEM((slots, seq), BF16),
        pltpu.VMEM((slots, cols), BF16),
        pltpu.VMEM((d, g.width), F32),
        pltpu.VMEM((d, g.width), F32),
        pltpu.VMEM(packets, BF16),
        pltpu.VMEM(packets, BF16),
        pltpu.VMEM((2, LANES, cols), BF16),
        pltpu.VMEM(packets, BF16),
        pltpu.VMEM(packets, BF16),
        pltpu.VMEM((g.chunks, rows, g.width), F32),
        pltpu.VMEM((nx, d // nx, LANES), F32),
        pltpu.VMEM((nx, d // nx, LANES), F32),
        pltpu.VMEM((nx, d // nx, LANES), F32),
        pltpu.VMEM((nx, d // nx, LANES), BF16),
        pltpu.VMEM((nx - 1, d // nx, LANES), BF16),
        pltpu.VMEM((g.per_x, g.per_t, room, LANES), BF16),
        pltpu.VMEM((g.nz, room, LANES), BF16),
        pltpu.SemaphoreType.REGULAR((8,)),
        dma((10,)),
        dma((2, half, 2 * g.chunks)),
        dma((2, half, 2 * g.chunks)),
        dma((2, half, 2 * g.chunks)),
        dma((2, half, 2 * g.chunks)),
        dma((2,)),
        dma((2,)),
        dma((2,)),
        dma((2,)),
        dma((nx,)),
        dma((nx,)),
        dma((nx,)),
        dma((nx - 1,)),
        dma,
        dma,
    ]
    features, grad = pl.pallas_call(
        functools.partial(kernel, g),
        out_shape=(
            jax.ShapeDtypeStruct(text_rows.shape, BF16),
            jax.ShapeDtypeStruct((g.each, rows), F32),
        ),
        in_specs=[hbm] * 10,
        out_specs=(vmem, vmem),
        scratch_shapes=scratch,
        compiler_params=pltpu.CompilerParams(collective_id=0, has_side_effects=True),
    )(
        patches,
        text_rows,
        cotangent,
        w_qkv,
        w_out,
        lengths,
        slot_plan,
        starts,
        ln_gain,
        ln_bias,
    )
    return features, grad.T


def solution(mesh, nx=4):
    groups = ("dp", "pipe")
    in_specs = (
        P("tensor", groups),
        P(groups),
        P(groups),
        P(groups),
        P("tensor", groups),
        P("tensor", groups),
        P(),
        P(),
        P(None, "tensor", None),
        P("tensor", None),
    )
    out_specs = (P("tensor", groups), P("tensor", groups))
    return jax.shard_map(
        functools.partial(shards, nx), mesh=mesh, in_specs=in_specs, out_specs=out_specs, check_vma=False
    )
```

```python
import functools
import math

import jax
import jax.numpy as jnp
from jax import lax
from jax.experimental import pallas as pl
from jax.experimental.pallas import tpu as pltpu
from jax.sharding import PartitionSpec as P

HEAD_DIM = 80
LANES = 128
EPSILON = 1e-06
F32 = jnp.float32
BF16 = jnp.bfloat16
MESH = pl.DeviceIdType.MESH


def dot(a, b, ca=1, cb=0):
    return lax.dot_general(a, b, (((ca,), (cb,)), ((), ())), preferred_element_type=F32)


def iota(shape, dim):
    return lax.broadcasted_iota(jnp.int32, shape, dim)


def kernel(
    g,
    patches_hbm,
    text_hbm,
    cot_hbm,
    wqkv_hbm,
    wout_hbm,
    lengths_hbm,
    slots_hbm,
    starts_hbm,
    gain_hbm,
    bias_hbm,
    features_hbm,
    grad_hbm,
    patches,
    text,
    cot,
    wqkv,
    wout,
    lengths_ref,
    slots_ref,
    starts_ref,
    gain_ref,
    bias_ref,
    xfull,
    cfull,
    w_split,
    w_full,
    onehot,
    pick,
    gainb,
    biasb,
    cot_out,
    cot_in,
    cot_sel,
    merged_out,
    merged_in,
    attended,
    grad_own,
    pair_out,
    pair_in,
    row_out,
    row_in,
    col_out,
    col_in,
    features,
    grad,
    low_out,
    low_in,
    onehot_low,
    pick_low,
    cover,
    store_sem,
    low_send,
    low_recv,
    near_sem,
    load_sem,
    xs_sem,
    xr_sem,
    cs_sem,
    cr_sem,
    a2a_send,
    a2a_recv,
    w_send,
    w_recv,
    pair_send,
    pair_recv,
    row_send,
    row_recv,
    col_send,
    col_recv,
):
    nx, nz, ny = g.nx, g.nz, g.ny
    ndp = nx * nz
    rows, width, chunks = g.rows, g.width, g.chunks
    cols = width * chunks
    length = g.length
    slots = ndp * length
    dp, y, c = lax.axis_index("dp"), lax.axis_index("tensor"), lax.axis_index("pipe")
    x, z = dp // nz, lax.rem(dp, nz)
    other = 1 - c

    loads = [
        pltpu.make_async_copy(a, b, load_sem.at[k])
        for k, (a, b) in enumerate(
            (
                (patches_hbm, patches),
                (cot_hbm, cot),
                (wout_hbm, wout),
                (wqkv_hbm, wqkv),
                (text_hbm, text),
                (lengths_hbm, lengths_ref.at[0]),
                (slots_hbm, slots_ref.at[0]),
                (starts_hbm, starts_ref.at[0]),
                (gain_hbm, gain_ref.at[0]),
                (bias_hbm, bias_ref.at[0]),
            )
        )
    ]
    for load in loads:
        load.start()

    def plane_peer(k):
        return (
            lax.rem(x + k // nz, nx) * nz + lax.rem(z + lax.rem(k + nz // 2, nz), nz),
            y,
            c,
        )

    phase = Phase()
    phase('greet')
    barrier = pltpu.get_barrier_semaphore()

    def signal(sem, device):
        pl.semaphore_signal(sem, inc=1, device_id=device, device_id_type=MESH)

    def place_at(dx, dz):
        return (lax.rem(x + dx, nx) * nz + lax.rem(z + dz, nz), y, c)

    signal(barrier, (dp, y, other))
    for way in (1, -1):
        signal(barrier, (dp, lax.rem(y + ny + way, ny), c))
        signal(barrier, place_at(0, nz + way))
        signal(barrier, place_at(nx + way, 0))
    phase('barrier_wait')
    pl.semaphore_wait(barrier, 7)

    rounds = []
    for count, axis in ((nz, 1), (nx, 0)):
        reach = 1
        while reach < count // 2:
            step = [(count + reach), (count - reach)]
            rounds.append([(0, r) if axis else (r, 0) for r in step])
            reach *= 2
    rounds.append([(r, 0) for r in range(1, nx)])

    def knock(n):
        for dx, dz in rounds[n]:
            signal(near_sem.at[n], place_at(dx, dz))

    def hear(n):
        pl.semaphore_wait(near_sem.at[n], len(rounds[n]))

    half = ny // 2
    parts = 2
    tall = rows // parts
    units = [(ch, h) for ch in range(chunks) for h in range(parts)]
    limits = {u: (half, ny - 1 - half) if n % 2 == 0 else (ny - 1 - half, half) for n, u in enumerate(units)}

    def hop(buf, ssem, rsem, way, step, unit):
        ch, h = unit
        if way == 0:
            origin, peer = lax.rem(y + ny - step, ny), lax.rem(y + 1, ny)
        else:
            origin, peer = lax.rem(y + step, ny), lax.rem(y + ny - 1, ny)
        piece = buf.at[ch, origin, pl.ds(h * tall, tall)]
        n = ch * parts + h
        return pltpu.make_async_remote_copy(
            src_ref=piece,
            dst_ref=piece,
            send_sem=ssem.at[way, step, n],
            recv_sem=rsem.at[way, step, n],
            device_id=(dp, peer, c),
            device_id_type=MESH,
        )

    hop_x = functools.partial(hop, xfull, xs_sem, xr_sem)
    hop_c = functools.partial(hop, cfull, cs_sem, cr_sem)

    def open_ring(hops, ch):
        for h in range(parts):
            for way in range(2):
                if limits[ch, h][way] > 0:
                    hops(way, 0, (ch, h)).start()

    def turn(hops, step, ch):
        for h in range(parts):
            for way in range(2):
                if step < limits[ch, h][way]:
                    hops(way, step, (ch, h)).wait_recv()
                    if step + 1 < limits[ch, h][way]:
                        hops(way, step + 1, (ch, h)).start()

    def close_ring(hops):
        for unit in units:
            for way in range(2):
                for step in range(limits[unit][way]):
                    hops(way, step, unit).wait_send()

    def exchange(arrays, low, high):
        count = high - low
        if count == 0:
            return

        def start(n, carry):
            peer = place_at(n // count, low + lax.rem(n, count))
            for send, recv, sent, got in arrays:
                pltpu.make_async_remote_copy(
                    src_ref=send.at[peer[0]],
                    dst_ref=recv.at[dp],
                    send_sem=sent,
                    recv_sem=got,
                    device_id=peer,
                    device_id_type=MESH,
                ).start()
            return carry

        lax.fori_loop(0 if low % nz else 1, nx * count, start, 0)

    def exchanged(arrays):
        part = pl.ds(0, ndp - 1)
        for send, recv, sent, got in arrays:
            pltpu.make_async_copy(recv.at[part], recv.at[part], got).wait()
            pltpu.make_async_copy(send.at[part], send.at[part], sent).wait()

    cot_arrays = ((cot_out, cot_in, a2a_send.at[0], a2a_recv.at[0]),)
    image_arrays = (
        (merged_out, merged_in, a2a_send.at[1], a2a_recv.at[1]),
        (low_out, low_in, low_send, low_recv),
    )

    phase('open_x')
    loads[0].wait()
    for ch in range(chunks):
        xfull[ch, y] = patches[:, ch * width : (ch + 1) * width]
        open_ring(hop_x, ch)
    z_rounds = 0
    while 2 ** (z_rounds + 1) <= nz // 2:
        z_rounds += 1
    last_round = len(rounds) - 1
    if z_rounds:
        knock(0)
    for n in range(z_rounds, last_round):
        knock(n)

    phase('cot_out')
    for load in loads[5:]:
        load.wait()
    place = iota((slots, ndp), 0) // length == iota((slots, ndp), 1)
    position = jnp.sum(
        jnp.where(place, starts_ref[...].astype(F32), 0.0), axis=1, keepdims=True
    ).astype(jnp.int32) + lax.rem(iota((slots, 1), 0), length)
    seq = g.seq
    onehot[...] = (iota((slots, seq), 1) == position).astype(F32).astype(BF16)
    place = lax.rem(iota((slots, ndp), 0), ndp) == iota((slots, ndp), 1)
    position = jnp.sum(
        jnp.where(place, starts_ref[...].astype(F32), 0.0), axis=1, keepdims=True
    ).astype(jnp.int32) + iota((slots, 1), 0) // ndp
    onehot_low[...] = (iota((slots, seq), 1) == position).astype(F32).astype(BF16)

    images = cols // length
    spread = (iota((images, cols), 1) // length == iota((images, cols), 0)).astype(F32).astype(BF16)

    def per_column(ref):
        values = jnp.broadcast_to(ref[...].astype(F32), (8, images)).astype(BF16)
        return dot(values, spread)[0:1].astype(jnp.int32)

    live_len = per_column(lengths_ref)
    within = lax.rem(iota((1, cols), 1), length)
    slot_of = per_column(slots_ref)
    live = within < live_len
    pick[...] = (iota((slots, cols), 0) == slot_of * length + within).astype(F32).astype(BF16)
    pick_low[...] = (iota((ndp, cols), 0) == slot_of).astype(F32).astype(BF16)
    loads[1].wait()
    each, room = g.each, LANES // g.per_t
    lined = iota((2 * LANES, rows), 0)
    rest = lax.rem(lined, LANES)
    column = (rest // room * 2 + lined // LANES) * each + lax.rem(rest, room)
    order = ((lax.rem(rest, room) < each) & (column == iota((2 * LANES, rows), 1))).astype(F32).astype(BF16)
    cot_lined = dot(order, cot[...]).astype(BF16)
    pair = [
        dot(onehot[...], cot_lined[k * LANES : (k + 1) * LANES], 1, 1).reshape(ndp, length, LANES)
        for k in range(2)
    ]
    flags = jnp.broadcast_to(jnp.where(live, 1.0, 0.0), (LANES, cols)).astype(BF16)
    flags = dot(pick[...], flags, 1, 1).reshape(ndp, length, LANES)
    pair[0] = jnp.where(iota((ndp, length, LANES), 2) == room - 1, flags, pair[0])
    cot_out[...] = jnp.concatenate(pair, axis=1).astype(BF16)
    cot_in[dp] = cot_out[dp]

    side = lax.rem(z, 2)

    def turn_weights():
        loads[2].wait()
        w_split[...] = wout[...].T.reshape(w_split.shape)
        w_full[c, side, y] = w_split[y, c, side]

    def spread_norm():
        gainb[...] = jnp.broadcast_to(gain_ref[...], (width, rows * ny)).T
        biasb[...] = jnp.broadcast_to(bias_ref[...], (width, rows * ny)).T

    def hear_axes():
        for n in range(z_rounds, last_round):
            hear(n)

    def next_round(n):
        hear(n)
        if n + 1 < z_rounds:
            knock(n + 1)
        else:
            hear_axes()
            knock(last_round)

    near = max(nz // 4, 1)

    def send_cotangent():
        hear(last_round)
        exchange(cot_arrays, near, nz - near + 1)

    def send_cotangent_rest():
        exchange(cot_arrays, nz - near + 1, nz)
        exchange(cot_arrays, 0, near)

    if z_rounds:
        next_round(0)
    else:
        hear_axes()
        knock(last_round)
    tasks = [turn_weights, None, spread_norm, None]
    for n in range(1, z_rounds):
        tasks[2 * n - 1] = functools.partial(next_round, n)
    tasks += [send_cotangent, send_cotangent_rest]

    for step in range(half - 1):
        for ch in range(chunks):
            phase('turn_x%d' % step)
            turn(hop_x, step, ch)
            if tasks:
                task = tasks.pop(0)
                phase('task_x%d_%d' % (step, ch))
                if task:
                    task()
    phase('rest_x')
    for task in tasks:
        if task:
            task()

    def w_copy(k):
        peer = lax.rem(y + k, ny)
        return pltpu.make_async_remote_copy(
            src_ref=w_split.at[peer, c, side],
            dst_ref=w_full.at[c, side, y],
            send_sem=w_send.at[0],
            recv_sem=w_recv.at[0],
            device_id=(dp, peer, c),
            device_id_type=MESH,
        )

    far_first = sorted(range(1, ny), key=lambda k: -min(k, ny - k))
    for k in far_first:
        if k != half:
            w_copy(k).start()
    w_beside = pltpu.make_async_remote_copy(
        src_ref=w_full.at[c, side],
        dst_ref=w_full.at[c, side],
        send_sem=w_send.at[2],
        recv_sem=w_recv.at[2],
        device_id=(dp + 1 - 2 * side, y, c),
        device_id_type=MESH,
    )
    w_pair = pltpu.make_async_remote_copy(
        src_ref=w_full.at[c],
        dst_ref=w_full.at[c],
        send_sem=w_send.at[1],
        recv_sem=w_recv.at[1],
        device_id=(dp, y, other),
        device_id_type=MESH,
    )
    loads[3].wait()
    key_row, query_col = iota((width, width), 0), iota((width, width), 1)
    same = key_row // length == query_col // length
    for ch in range(chunks):
        phase('turn_x_last_%d' % ch)
        turn(hop_x, half - 1, ch)
        if ch == 0:
            w_copy(half).start()
        phase('attention_%d' % ch)
        here = slice(ch * width, (ch + 1) * width)
        inputs = xfull[ch].reshape(ny * rows, width).astype(F32)
        centred = inputs - jnp.mean(inputs, axis=0, keepdims=True)
        variance = jnp.mean(centred * centred, axis=0, keepdims=True)
        normed = (centred * lax.rsqrt(variance + EPSILON) * gainb[...] + biasb[...]).astype(BF16)
        queries, keys, values = (dot(wqkv[k], normed).astype(BF16) for k in range(3))
        mask = same & (lax.rem(key_row, length) < live_len[:, here])
        contexts = []
        for head in range(rows // HEAD_DIM):
            part = slice(head * HEAD_DIM, (head + 1) * HEAD_DIM)
            scores = dot(keys[part], queries[part], 0, 0) * (1.0 / math.sqrt(HEAD_DIM))
            scores = jnp.where(mask, scores, -1e30)
            raised = jnp.exp(scores - jnp.max(scores, axis=0, keepdims=True))
            weights = (raised / jnp.sum(raised, axis=0, keepdims=True)).astype(BF16)
            contexts.append(dot(values[part], weights))
        context = jnp.concatenate(contexts, axis=0)
        cfull[ch, y] = jnp.where(live[:, here], context, 0.0).astype(BF16)
        open_ring(hop_c, ch)
    phase('close_x')
    close_ring(hop_x)

    arrivals = [0]
    for away in range(1, half + 1):
        arrivals += [away, ny - away] if away < half else [away]
    per_x = g.per_x
    shares = [arrivals[k * per_x : (k + 1) * per_x] for k in range(nx)]
    ready = [max(max(min(a, ny - a) for a in share) - 1, 0) for share in shares]
    home_x = y * g.per_t // nz
    mine = lax.rem(x + nx - home_x + nx // 2, nx)

    def block_at(away):
        return lax.rem(y + away, ny)

    def project(away):
        at = block_at(away)
        weights = jnp.concatenate([w_full[k // 2, k % 2, at] for k in range(4)], axis=0)
        for ch in range(chunks):
            piece = dot(weights, cfull[ch, at]).astype(BF16).astype(F32)
            attended[ch] = piece if away == 0 else attended[ch] + piece

    def pair_copy(k):
        return pltpu.make_async_remote_copy(
            src_ref=pair_out.at[k],
            dst_ref=pair_in.at[k],
            send_sem=pair_send.at[k],
            recv_sem=pair_recv.at[k],
            device_id=(dp, y, other),
            device_id_type=MESH,
        )

    def term(k, side):
        blocks = []
        for away in shares[k]:
            total = jnp.zeros((rows, LANES), F32)
            for ch in range(chunks):
                block = cot_sel[side, :, ch * width : (ch + 1) * width]
                total += dot(cfull[ch, block_at(away)], block, 1, 1)
            blocks.append(total)
        return jnp.concatenate(blocks, axis=0)

    def first_stage(k):
        pair_out[k] = term(k, other)
        pair_copy(k).start()
        grad_own[k] = term(k, c)

    def row_copy(k):
        peer = lax.rem(home_x + k + nx - nx // 2, nx)
        slot = lax.rem(peer - x + nx + nx - 1, nx)
        return pltpu.make_async_remote_copy(
            src_ref=row_out.at[k],
            dst_ref=row_in.at[slot],
            send_sem=row_send.at[k],
            recv_sem=row_recv.at[slot],
            device_id=(peer * nz + z, y, c),
            device_id_type=MESH,
        )

    def second_stage(k):
        pair_copy(k).wait()
        total = grad_own[k] + pair_in[k]
        grad_own[k] = total
        row_out[k] = total.astype(BF16)

        @pl.when(mine != k)
        def _():
            row_copy(k).start()

    def column_copy(b, target, away):
        return pltpu.make_async_remote_copy(
            src_ref=col_out.at[b, target],
            dst_ref=col_in.at[z],
            send_sem=col_send,
            recv_sem=col_recv,
            device_id=(y * g.per_t + target, block_at(away), c),
            device_id_type=MESH,
        )

    over = rows - LANES

    def third_stage(k):
        @pl.when(mine == k)
        def _():
            total = grad_own[k]
            for slot in range(nx - 1):
                arrived = pltpu.make_async_copy(row_in.at[slot], row_in.at[slot], row_recv.at[slot])
                arrived.wait()
                total += row_in[slot].astype(F32)
            for b, away in enumerate(shares[k]):
                turned = total[b * rows : (b + 1) * rows].T.reshape(g.per_t, room, rows)
                tail = turned[:, :each, LANES:]
                spare = jnp.zeros((g.per_t, each // 2, LANES - 2 * over), F32)
                tail = jnp.concatenate([tail[:, : each // 2], tail[:, each // 2 :], spare], axis=2)
                spare = jnp.zeros((g.per_t, room - each - each // 2, LANES), F32)
                packed = jnp.concatenate([turned[:, :each, :LANES], tail, spare], axis=1)
                col_out[b] = packed.astype(BF16)

                def send(target, carry, b=b, away=away):
                    column_copy(b, target, away).start()
                    return carry

                lax.fori_loop(0, g.per_t, send, 0)

    def select_cotangent():
        exchanged(cot_arrays)
        arrived = cot_in[...].astype(F32)
        for k in range(2):
            block = arrived[:, k * length : (k + 1) * length].reshape(slots, LANES).astype(BF16)
            cot_sel[k] = dot(block, pick[...], 0, 0).astype(BF16)

    def find_cover():
        block = cot_in[...].astype(F32)[:, :length].reshape(slots, LANES).T
        cover[...] = dot(block[room - 8 : room].astype(BF16), onehot[...])

    def take_weights():
        mine_only = w_full.at[c, side, pl.ds(0, ny - 1)]
        pltpu.make_async_copy(mine_only, mine_only, w_recv.at[0]).wait()
        pltpu.make_async_copy(mine_only, mine_only, w_send.at[0]).wait()
        w_beside.start()

    def pair_weights():
        w_beside.wait()
        w_pair.start()

    def between(k):
        def run():
            second_stage(k - 1)
            if k == 1:
                w_pair.wait()
            for away in shares[k - 1]:
                project(away)

        return run

    tasks = [(-1, take_weights), (0, None), (0, select_cotangent), (ready[0], functools.partial(first_stage, 0))]
    tasks.append((0, pair_weights))
    for k in range(1, nx):
        tasks += [(ready[k], functools.partial(first_stage, k)), (ready[k], between(k))]
    for step in range(half):
        for ch in range(chunks):
            phase('turn_c%d' % step)
            turn(hop_c, step, ch)
            done = step if ch == chunks - 1 else step - 1
            if tasks and tasks[0][0] <= done and (step < half - 1 or ch < chunks - 1):
                phase('task_c%d_%d' % (step, ch))
                task = tasks.pop(0)[1]
                if task:
                    task()
    phase('rest_c')
    for _, task in tasks:
        if task:
            task()
    for away in shares[-1]:
        project(away)
    for k in range(nx - 2):
        phase('third_%d' % k)
        third_stage(k)

    phase('merged_out')
    pieces = []
    for ch in range(chunks):
        here = slice(ch * width, (ch + 1) * width)
        merged = patches[:, here].astype(F32) + attended[ch].astype(BF16).astype(F32)
        pieces.append(merged.astype(BF16))
    merged = jnp.concatenate(pieces, axis=1)
    upper = dot(pick[...], merged[:LANES], 1, 1).reshape(ndp, length, LANES)
    merged_out[...] = upper.astype(BF16)
    group = LANES // over
    for r in range(2):
        spots = [
            jnp.where(within == r * group + q, merged[LANES:].astype(F32), 0.0).astype(BF16)
            for q in range(group)
        ]
        low_out[:, r, :] = dot(pick_low[...], jnp.concatenate(spots, axis=0), 1, 1)
    merged_in[dp] = merged_out[dp]
    low_in[dp] = low_out[dp]
    phase('pair_last')
    second_stage(nx - 1)
    phase('merged_send')
    exchange(image_arrays, near, nz - near + 1)
    phase('third_last')
    third_stage(nx - 2)
    third_stage(nx - 1)
    phase('merged_send2')
    exchange(image_arrays, nz - near + 1, nz)
    exchange(image_arrays, 0, near)
    phase('cover')
    find_cover()
    loads[4].wait()
    close_ring(hop_c)
    for k in range(nx):
        @pl.when(mine != k)
        def _(k=k):
            row_copy(k).wait_send()

    phase('merged_wait')
    exchanged(image_arrays)
    phase('place')
    first = merged_in[...].astype(F32).reshape(slots, LANES).T.astype(BF16)
    second = [
        low_in[:, j // group, :][:, j % group * over : (j % group + 1) * over] for j in range(length)
    ]
    second = jnp.concatenate(second, axis=0).T.astype(BF16)
    wide = g.seq_block
    stores = []
    for k in range(seq // wide):
        here = slice(k * wide, (k + 1) * wide)
        upper, lower = dot(first, onehot[:, here]), dot(second, onehot_low[:, here])
        placed = jnp.concatenate([upper, lower], axis=0).astype(BF16)
        features[:, here] = jnp.where(cover[7:8, here] > 0.5, placed, text[:, here])
        part = pl.ds(k * wide, wide)
        stores.append(
            pltpu.make_async_copy(features.at[:, part], features_hbm.at[:, part], store_sem.at[1 + k])
        )
        stores[-1].start()

    phase('col_wait')
    pltpu.make_async_copy(col_in, col_in, col_recv).wait()
    pltpu.make_async_copy(col_out, col_out, col_send).wait()
    phase('finish')
    total = jnp.sum(col_in[...].astype(F32), axis=0)
    tail = total[each : each + each // 2]
    tail = jnp.concatenate([tail[:, :over], tail[:, over : 2 * over]], axis=0)
    grad[...] = jnp.concatenate([total[:each], tail], axis=1)
    stores.append(pltpu.make_async_copy(grad, grad_hbm, store_sem.at[0]))
    stores[-1].start()
    for store in stores:
        store.wait()
    phase(None)


class Phase:
    scope = None

    def __call__(self, name):
        if self.scope is not None:
            self.scope.__exit__(None, None, None)
        self.scope = jax.named_scope(name) if name else None
        if name:
            self.scope.__enter__()


class Geometry:
    def __init__(self, nx, nz, ny, rows, cols, images, seq):
        self.nx, self.nz, self.ny, self.rows = nx, nz, ny, rows
        self.length = cols // images
        self.chunks = 3
        self.width = cols // self.chunks
        self.seq = seq
        self.seq_block = 256 if seq % 256 == 0 else seq
        self.per_t, self.per_x = nx * nz // ny, ny // nx
        self.each = rows * ny // (nx * nz * 2)


def shards(nx, patches, lengths, slot_plan, starts, text_rows, cotangent, ln_gain, ln_bias, w_qkv, w_out):
    ndp, ny = lax.axis_size("dp"), lax.axis_size("tensor")
    rows, cols = patches.shape
    d = w_out.shape[1]
    seq = text_rows.shape[1]
    g = Geometry(nx, ndp // nx, ny, rows, cols, lengths.shape[0], seq)
    slots = ndp * g.length
    room = LANES // g.per_t
    half = max(ny // 2, 1)
    hbm = pl.BlockSpec(memory_space=pl.ANY)
    dma = pltpu.SemaphoreType.DMA
    ring = (g.chunks, ny, rows, g.width)
    packets = (ndp, 2 * g.length, LANES)
    scratch = [
        pltpu.VMEM(patches.shape, BF16),
        pltpu.VMEM(text_rows.shape, BF16),
        pltpu.VMEM(cotangent.shape, BF16),
        pltpu.VMEM(w_qkv.shape, BF16),
        pltpu.VMEM(w_out.shape, BF16),
        pltpu.VMEM((1,) + lengths.shape, jnp.int32),
        pltpu.VMEM((1,) + slot_plan.shape, jnp.int32),
        pltpu.VMEM((1,) + starts.shape, jnp.int32),
        pltpu.VMEM((1,) + ln_gain.shape, F32),
        pltpu.VMEM((1,) + ln_bias.shape, F32),
        pltpu.VMEM(ring, BF16),
        pltpu.VMEM(ring, BF16),
        pltpu.VMEM((ny, 2, 2, rows // 4, rows), BF16),
        pltpu.VMEM((2, 2, ny, rows // 4, rows), BF16),
        pltpu.VMEM((slots, seq), BF16),
        pltpu.VMEM((slots, cols), BF16),
        pltpu.VMEM((d, g.width), F32),
        pltpu.VMEM((d, g.width), F32),
        pltpu.VMEM(packets, BF16),
        pltpu.VMEM(packets, BF16),
        pltpu.VMEM((2, LANES, cols), BF16),
        pltpu.VMEM((ndp, g.length, LANES), BF16),
        pltpu.VMEM((ndp, g.length, LANES), BF16),
        pltpu.VMEM((g.chunks, rows, g.width), F32),
        pltpu.VMEM((nx, d // nx, LANES), F32),
        pltpu.VMEM((nx, d // nx, LANES), F32),
        pltpu.VMEM((nx, d // nx, LANES), F32),
        pltpu.VMEM((nx, d // nx, LANES), BF16),
        pltpu.VMEM((nx - 1, d // nx, LANES), BF16),
        pltpu.VMEM((g.per_x, g.per_t, room, LANES), BF16),
        pltpu.VMEM((g.nz, room, LANES), BF16),
        pltpu.VMEM(text_rows.shape, BF16),
        pltpu.VMEM((g.each, rows), F32),
        pltpu.VMEM((ndp, 2, LANES), F32),
        pltpu.VMEM((ndp, 2, LANES), F32),
        pltpu.VMEM((slots, seq), BF16),
        pltpu.VMEM((ndp, cols), BF16),
        pltpu.VMEM((8, seq), F32),
        dma((1 + seq // g.seq_block,)),
        dma,
        dma,
        pltpu.SemaphoreType.REGULAR((8,)),
        dma((10,)),
        dma((2, half, 2 * g.chunks)),
        dma((2, half, 2 * g.chunks)),
        dma((2, half, 2 * g.chunks)),
        dma((2, half, 2 * g.chunks)),
        dma((2,)),
        dma((2,)),
        dma((3,)),
        dma((3,)),
        dma((nx,)),
        dma((nx,)),
        dma((nx,)),
        dma((nx - 1,)),
        dma,
        dma,
    ]
    features, grad = pl.pallas_call(
        functools.partial(kernel, g),
        out_shape=(
            jax.ShapeDtypeStruct(text_rows.shape, BF16),
            jax.ShapeDtypeStruct((g.each, rows), F32),
        ),
        in_specs=[hbm] * 10,
        out_specs=(hbm, hbm),
        scratch_shapes=scratch,
        compiler_params=pltpu.CompilerParams(collective_id=0, has_side_effects=True),
    )(
        patches,
        text_rows,
        cotangent,
        w_qkv,
        w_out,
        lengths,
        slot_plan,
        starts,
        ln_gain,
        ln_bias,
    )
    return features, grad.T


def solution(mesh, nx=4):
    groups = ("dp", "pipe")
    in_specs = (
        P("tensor", groups),
        P(groups),
        P(groups),
        P(groups),
        P("tensor", groups),
        P("tensor", groups),
        P(),
        P(),
        P(None, "tensor", None),
        P("tensor", None),
    )
    out_specs = (P("tensor", groups), P("tensor", groups))
    return jax.shard_map(
        functools.partial(shards, nx), mesh=mesh, in_specs=in_specs, out_specs=out_specs, check_vma=False
    )
```
